32 devices in a mesh: gx: 8 (over z, core), gy: 4 (over y, x).
Axes of the slice: x: 2, y: 2, z: 4, core: 2. Of those that a mesh axis runs over, the one named last changes fastest.
Arguments:
- green: bfloat16 [8, 4, 1024, 1024], P('gx', 'gy'), may hold values from -0.1875 to 0.1875
- sources: bfloat16 [6, 8, 4, 768, 128], P(None, 'gx', 'gy'), may hold values from -3 to 3
- entering: float32 [8, 4, 1024, 128], P('gx', 'gy'), may hold values from -6 to 6
- start_front: int32 [6], replicated, may hold values from -5 to 5, as said below
Outputs:
- last_traces: float32 [8, 4, 1024, 128], P('gx', 'gy')
The draws below stay inside these ranges and needn't reach their ends.
Inputs may be any that keep to these rules, and one draw needn't show every extreme that they name: `start_front`: the 6 values are distinct.
All inputs are finite; a program needn't handle non-finite values.
Results may differ from the reference program's by a relative error of at most 0.0055.
Values may be sent and summed in bfloat16 or wider, within the bound.
No kernel may reach another device: no remote copies, remote signals or barrier semaphores. Data moves between devices by JAX's collectives and lax.ppermute only.
A program may use at most 64 MiB of HBM per device.

```python
import jax
import jax.numpy as jnp
from jax import lax

TRACE = 384
BS = 128
TICKS = 6
ORDER = 1024
FRONTS = 11
NB = 6
N_GX = 8
N_GY = 4


def draw_start_front(key, part):
    shuffled = jax.random.permutation(key, FRONTS)
    return (shuffled[:NB] + (1 - TICKS)).astype(jnp.int32)


def shard_levels(stream_key, shape, cuts, low, top_value):
    loudness, own = 1.0, jax.random.fold_in(stream_key, 6)
    for position, parts in cuts:
        draws = jnp.exp(jax.random.uniform(jax.random.fold_in(own, position), (parts,), jnp.float32, low / len(cuts), top_value / len(cuts)))
        loudness = loudness * jnp.repeat(draws, shape[position] // parts).reshape([-1 if axis == position else 1 for axis in range(len(shape))])
    return loudness


def normal_values(stream_key, extent, scale, reach, cuts=(), kind=jnp.bfloat16):
    gain = shard_levels(stream_key, extent, cuts, -0.22, 0.18) if cuts else 1.0
    result = jax.random.normal(stream_key, extent, jnp.float32) * scale * gain
    return jnp.minimum(jnp.maximum(result, -reach), reach).astype(kind)


def setup_inputs(seed: int = 0) -> dict:
    arg_keys = jax.random.split(jax.random.key(seed), 5)
    green = normal_values(arg_keys[0], (N_GX, N_GY, ORDER, ORDER), ORDER ** -0.5, 0.1875, ((0, 8), (1, 4)))
    sources = normal_values(arg_keys[1], (TICKS, N_GX, N_GY, 2 * TRACE, BS), 0.5, 3.0, ((1, 8), (2, 4)))
    entering = normal_values(arg_keys[2], (N_GX, N_GY, ORDER, BS), 1.0, 6.0, ((0, 8), (1, 4)), jnp.float32)
    start_front = draw_start_front(jax.random.fold_in(arg_keys[4], 71), 0)
    return dict(green=green, sources=sources, entering=entering, start_front=start_front)


def apply_row(operands):
    operator_row, rounded_row = operands
    return jnp.einsum("joi,jib->job", operator_row.astype(jnp.float32), rounded_row.astype(jnp.float32))


def reference(green, sources, entering, start_front):
    column_total = green.shape[0]
    row_total = green.shape[1]
    edge_rows = sources.shape[3]
    trace_rows = edge_rows // 2
    corner_rows = green.shape[2] - edge_rows
    width = entering.shape[3]
    front_map = (jnp.arange(column_total, dtype=jnp.int32)[:, None] + jnp.arange(row_total, dtype=jnp.int32)[None, :])
    incoming = entering
    traces = entering
    for step_index in range(TICKS):
        if step_index > 0:
            east_part = traces[:, :, :trace_rows]
            north_part = traces[:, :, trace_rows:edge_rows]
            corner_part = traces[:, :, edge_rows:]
            west_in = jnp.pad(east_part, ((1, 0), (0, 0), (0, 0), (0, 0)))[:-1]
            south_in = jnp.pad(north_part, ((0, 0), (1, 0), (0, 0), (0, 0)))[:, :-1]
            diagonal = jnp.pad(corner_part, ((1, 0), (1, 0), (0, 0), (0, 0)))[:-1, :-1]
            incoming = jnp.concatenate([west_in, south_in, diagonal], axis=2)
        rounded = incoming.astype(jnp.bfloat16)
        product = lax.map(apply_row, (green, rounded))
        source_term = jnp.concatenate([sources[step_index].astype(jnp.float32), jnp.zeros((column_total, row_total, corner_rows, width), jnp.float32)], axis=2)
        is_live = jnp.any(start_front[None, None, :] == (front_map - step_index)[:, :, None], axis=-1)
        traces = jnp.where(is_live[:, :, None, None], product + source_term, jnp.zeros_like(product))
    return traces
```

```python
import jax
import jax.numpy as jnp
from jax import lax
from jax.sharding import PartitionSpec as P

AXES = ("gx", "gy")


def passed_along(shard, dx, dy):
    nx, ny = lax.axis_size("gx"), lax.axis_size("gy")
    pairs = [
        (i * ny + j, (i + dx) % nx * ny + (j + dy) % ny)
        for i in range(nx)
        for j in range(ny)
    ]
    return lax.ppermute(shard, AXES, pairs)


def local(green, sources, entering, start_front):
    operator = green[0, 0]
    tick_total = sources.shape[0]
    edge_rows = sources.shape[3]
    trace_rows = edge_rows // 2
    corner_rows = operator.shape[0] - edge_rows
    width = entering.shape[3]
    column, row = lax.axis_index("gx"), lax.axis_index("gy")
    front_index = column + row
    rounded = entering[0, 0].astype(jnp.bfloat16)
    corner_zeros = jnp.zeros((corner_rows, width), jnp.float32)
    traces = entering[0, 0]

    def kept(arrived, inside):
        return jnp.where(inside, arrived, jnp.zeros_like(arrived))

    for step_index in range(tick_total):
        if step_index > 0:
            outgoing = traces.astype(jnp.bfloat16)
            diagonal = passed_along(outgoing[edge_rows:], 1, 1)
            west_in = passed_along(outgoing[:trace_rows], 1, 0)
            south_in = passed_along(outgoing[trace_rows:edge_rows], 0, 1)
            rounded = jnp.concatenate(
                [
                    kept(west_in, column > 0),
                    kept(south_in, row > 0),
                    kept(diagonal, (column > 0) & (row > 0)),
                ],
                axis=0,
            )
        product = jnp.dot(operator, rounded, preferred_element_type=jnp.float32)
        source_term = jnp.concatenate(
            [sources[step_index, 0, 0].astype(jnp.float32), corner_zeros], axis=0
        )
        is_live = jnp.any(start_front == front_index - step_index)
        traces = jnp.where(is_live, product + source_term, jnp.zeros_like(product))
    return traces[None, None]


def solution(mesh):
    in_specs = (
        P("gx", "gy", None, None),
        P(None, "gx", "gy", None, None),
        P("gx", "gy", None, None),
        P(),
    )
    out_specs = P("gx", "gy", None, None)
    return jax.shard_map(local, mesh=mesh, in_specs=in_specs, out_specs=out_specs, check_vma=False)
```

```python
import random

import jax
import jax.numpy as jnp
from jax import lax
from jax.sharding import PartitionSpec as P

AXES = ("gx", "gy")


def distance(mesh, a, b):
    devices = mesh.devices.flat
    place = []
    for k in (a, b):
        coords = getattr(devices[k], "coords", None)
        place.append(divmod(k, mesh.shape["gy"]) if coords is None else tuple(coords))
    return sum(abs(p - q) for p, q in zip(*place))


def shift_pairs(mesh, dx, dy):
    nx, ny = mesh.shape["gx"], mesh.shape["gy"]
    return [(i * ny + j, (i + dx) % nx * ny + (j + dy) % ny) for i in range(nx) for j in range(ny)]


def diagonal_pairs(mesh):
    nx, ny = mesh.shape["gx"], mesh.shape["gy"]
    inner = [(i * ny + j, (i + 1) * ny + j + 1) for i in range(nx - 1) for j in range(ny - 1)]
    onward = dict(inner)
    arrived = set(onward.values())
    starts = [k for k in range(nx * ny) if k not in arrived]
    ends = []
    for k in starts:
        while k in onward:
            k = onward[k]
        ends.append(k)
    total = len(starts)
    gap = [[distance(mesh, e, s) for s in starts] for e in ends]

    def cost(order):
        hops = [gap[order[k - 1]][order[k]] for k in range(total)]
        return max(hops), sum(h * h for h in hops)

    draw = random.Random(1)
    best = None
    for _ in range(max(1, 6000 // total**2)):
        order = list(range(total))
        draw.shuffle(order)
        current = cost(order)
        moved = True
        while moved:
            moved = False
            for a in range(total):
                for b in range(a + 1, total):
                    swapped = order[:]
                    swapped[a], swapped[b] = swapped[b], swapped[a]
                    slid = order[:a] + order[a + 1 : b + 1] + [order[a]] + order[b + 1 :]
                    for trial in (swapped, slid):
                        value = cost(trial)
                        if value < current:
                            order, current, moved = trial, value, True
        if best is None or current < best[0]:
            best = current, order
    order = best[1]
    return inner + [(ends[order[k - 1]], starts[order[k]]) for k in range(total)]


def after(value, *others):
    return lax.optimization_barrier((value, *others))[0]


def local(pairs, green, sources, entering, start_front):
    operator = green[0, 0]
    tick_total = sources.shape[0]
    order = operator.shape[0]
    edge_rows = sources.shape[3]
    trace_rows = edge_rows // 2
    width = entering.shape[3]
    column, row = lax.axis_index("gx"), lax.axis_index("gy")
    column_total, row_total = lax.axis_size("gx"), lax.axis_size("gy")
    front_index = column + row
    rows = {"east": slice(0, trace_rows), "north": slice(trace_rows, edge_rows), "corner": slice(edge_rows, order)}
    has_target = {"east": column < column_total - 1, "north": row < row_total - 1}
    has_target["corner"] = has_target["east"] & has_target["north"]
    has_source = {"east": column > 0, "north": row > 0}
    has_source["corner"] = has_source["east"] & has_source["north"]

    def times(matrix, vectors):
        return jnp.dot(matrix, vectors, preferred_element_type=jnp.float32)

    def source_term(step_index):
        edges = sources[step_index, 0, 0].astype(jnp.float32)
        return jnp.concatenate([edges, jnp.zeros((order - edge_rows, width), jnp.float32)], axis=0)

    def kept(condition, value):
        return jnp.where(condition, value, jnp.zeros_like(value))

    first = times(operator, entering[0, 0].astype(jnp.bfloat16)) + source_term(0)
    first = first.astype(jnp.bfloat16)
    outgoing = {name: first[rows[name]] for name in ("corner", "east", "north")}

    span = max(tick_total, 3)
    age = front_index - after(start_front, outgoing["north"])
    live_bits = lax.reduce(
        jnp.where((age >= 0) & (age < span), lax.shift_left(jnp.int32(1), jnp.clip(age, 0, span - 1)), 0),
        jnp.int32(0),
        lax.bitwise_or,
        (0,),
    )
    live_bits = live_bits | (front_index << span)

    def live(step_index):
        return (lax.shift_right_logical(live_bits, jnp.int32(step_index)) & 1) == 1

    for step_index in range(1, tick_total):
        arrived = {name: lax.ppermute(outgoing[name], AXES, pairs[name]) for name in ("corner", "east", "north")}
        if step_index == 1:
            has_source["corner"] = has_source["corner"] & live(2)
            arrived = {name: kept(has_source[name], value) for name, value in arrived.items()}
        partial = source_term(step_index)
        for name in ("east", "corner"):
            partial = partial + times(operator[:, rows[name]], arrived[name])
        if step_index == tick_total - 1:
            total = times(operator[:, rows["north"]], arrived["north"]) + partial
            return kept(live(step_index), total)[None, None]
        outgoing, previous = {}, arrived["north"]
        for name in ("corner", "east", "north"):
            product = times(operator[rows[name], rows["north"]], previous) + partial[rows[name]]
            sent = has_target[name] & live(step_index) if name == "corner" else has_target[name]
            outgoing[name] = kept(sent, product).astype(jnp.bfloat16)
            previous = after(arrived["north"], outgoing[name])


def solution(mesh):
    pairs = {
        "east": shift_pairs(mesh, 1, 0),
        "north": shift_pairs(mesh, 0, 1),
        "corner": diagonal_pairs(mesh),
    }
    in_specs = (
        P("gx", "gy", None, None),
        P(None, "gx", "gy", None, None),
        P("gx", "gy", None, None),
        P(),
    )

    def body(*shards):
        return local(pairs, *shards)

    return jax.shard_map(body, mesh=mesh, in_specs=in_specs, out_specs=P("gx", "gy", None, None), check_vma=False)
```

```python
import random

import jax
import jax.numpy as jnp
from jax import lax
from jax.experimental import pallas as pl
from jax.experimental.pallas import tpu as pltpu
from jax.sharding import PartitionSpec as P

AXES = ("gx", "gy")
SENT = ("corner", "east", "north")


def distance(mesh, a, b):
    devices = mesh.devices.flat
    place = []
    for k in (a, b):
        coords = getattr(devices[k], "coords", None)
        place.append(divmod(k, mesh.shape["gy"]) if coords is None else tuple(coords))
    return sum(abs(p - q) for p, q in zip(*place))


def shift_pairs(mesh, dx, dy):
    nx, ny = mesh.shape["gx"], mesh.shape["gy"]
    return [(i * ny + j, (i + dx) % nx * ny + (j + dy) % ny) for i in range(nx) for j in range(ny)]


def diagonal_pairs(mesh):
    nx, ny = mesh.shape["gx"], mesh.shape["gy"]
    inner = [(i * ny + j, (i + 1) * ny + j + 1) for i in range(nx - 1) for j in range(ny - 1)]
    onward = dict(inner)
    arrived = set(onward.values())
    starts = [k for k in range(nx * ny) if k not in arrived]
    ends = []
    for k in starts:
        while k in onward:
            k = onward[k]
        ends.append(k)
    total = len(starts)
    gap = [[distance(mesh, e, s) for s in starts] for e in ends]

    def cost(order):
        hops = [gap[order[k - 1]][order[k]] for k in range(total)]
        return max(hops), sum(h * h for h in hops)

    draw = random.Random(1)
    best = None
    for _ in range(max(1, 6000 // total**2)):
        order = list(range(total))
        draw.shuffle(order)
        current = cost(order)
        moved = True
        while moved:
            moved = False
            for a in range(total):
                for b in range(a + 1, total):
                    swapped = order[:]
                    swapped[a], swapped[b] = swapped[b], swapped[a]
                    slid = order[:a] + order[a + 1 : b + 1] + [order[a]] + order[b + 1 :]
                    for trial in (swapped, slid):
                        value = cost(trial)
                        if value < current:
                            order, current, moved = trial, value, True
        if best is None or current < best[0]:
            best = current, order
    order = best[1]
    return inner + [(ends[order[k - 1]], starts[order[k]]) for k in range(total)]


def after(value, *others):
    return lax.optimization_barrier((value, *others))[0]


def trace_slices(order, edge_rows):
    trace_rows = edge_rows // 2
    return {
        "east": slice(0, trace_rows),
        "north": slice(trace_rows, edge_rows),
        "corner": slice(edge_rows, order),
    }


def targets():
    east = lax.axis_index("gx") < lax.axis_size("gx") - 1
    north = lax.axis_index("gy") < lax.axis_size("gy") - 1
    return {"east": east, "north": north, "corner": east & north}


def first_tick(green, sources, entering):
    order, width = entering.shape[2:]
    edge_rows = sources.shape[3]
    rows = trace_slices(order, edge_rows)

    def kernel(green_hbm, sources_hbm, entering_hbm, corner, east, north, operator, later, edges, wide, narrow, sems):
        outgoing = {"corner": corner, "east": east, "north": north}
        has_target = targets()

        def fetch(source, target, k):
            copy = pltpu.make_async_copy(source, target, sems.at[k])
            copy.start()
            return copy

        entering_copy = fetch(entering_hbm.at[0, 0], wide, 0)
        operator_copies = {}
        for k, name in enumerate(SENT):
            part = pl.ds(rows[name].start, rows[name].stop - rows[name].start)
            operator_copies[name] = fetch(green_hbm.at[0, 0, part], operator.at[part], 1 + k)
            if k == 0:
                edges_copy = fetch(sources_hbm.at[0, 0, 0], edges, 1 + len(SENT))
        later_copy = fetch(sources_hbm.at[1, 0, 0], later, 2 + len(SENT))
        entering_copy.wait()
        narrow[...] = wide[...].astype(jnp.bfloat16)
        for name in SENT:
            operator_copies[name].wait()
            product = jnp.dot(operator[rows[name]], narrow[...], preferred_element_type=jnp.float32)
            if name == SENT[1]:
                edges_copy.wait()
            if name != "corner":
                product = product + edges[rows[name]].astype(jnp.float32)
            outgoing[name][...] = jnp.where(has_target[name], product, 0.0).astype(jnp.bfloat16)
        later_copy.wait()

    count = {name: rows[name].stop - rows[name].start for name in SENT}
    results = [jax.ShapeDtypeStruct((count[name], width), jnp.bfloat16) for name in SENT]
    results += [jax.ShapeDtypeStruct((order, order), jnp.bfloat16), jax.ShapeDtypeStruct((edge_rows, width), jnp.bfloat16)]
    call = pl.pallas_call(
        kernel,
        out_shape=results,
        in_specs=[pl.BlockSpec(memory_space=pltpu.HBM)] * 3,
        out_specs=[pl.BlockSpec(memory_space=pltpu.VMEM)] * len(results),
        scratch_shapes=[
            pltpu.VMEM((edge_rows, width), jnp.bfloat16),
            pltpu.VMEM((order, width), jnp.float32),
            pltpu.VMEM((order, width), jnp.bfloat16),
            pltpu.SemaphoreType.DMA((3 + len(SENT),)),
        ],
        compiler_params=pltpu.CompilerParams(vmem_limit_bytes=46_000_000),
        cost_estimate=pl.CostEstimate(
            flops=2 * order * order * width,
            bytes_accessed=2 * order * order + 4 * order * width + 4 * edge_rows * width,
            transcendentals=0,
        ),
        name="first_tick",
    )
    in_hbm = [pltpu.with_memory_space_constraint(value, pltpu.HBM) for value in (green, sources, entering)]
    *outgoing, operator, later = call(*in_hbm)
    return dict(zip(SENT, outgoing)), operator, later


def local(pairs, green, sources, entering, start_front):
    tick_total = sources.shape[0]
    order, width = entering.shape[2:]
    edge_rows = sources.shape[3]
    rows = trace_slices(order, edge_rows)
    front_index = lax.axis_index("gx") + lax.axis_index("gy")
    has_target = targets()

    def times(matrix, vectors):
        return jnp.dot(matrix, vectors, preferred_element_type=jnp.float32)

    def source_term(edges):
        return jnp.concatenate(
            [edges.astype(jnp.float32), jnp.zeros((order - edge_rows, width), jnp.float32)], axis=0
        )

    def kept(condition, value):
        return jnp.where(condition, value, jnp.zeros_like(value))

    outgoing, operator, second_edges = first_tick(green, sources, entering)

    span = max(tick_total, 3)
    age = front_index - after(start_front, outgoing["north"])
    live_bits = lax.reduce(
        jnp.where((age >= 0) & (age < span), lax.shift_left(jnp.int32(1), jnp.clip(age, 0, span - 1)), 0),
        jnp.int32(0),
        lax.bitwise_or,
        (0,),
    )
    live_bits = live_bits | (front_index << span)
    later_sources = after(sources, outgoing["north"])

    def live(step_index):
        return (lax.shift_right_logical(live_bits, jnp.int32(step_index)) & 1) == 1

    for step_index in range(1, tick_total):
        arrived = {name: lax.ppermute(outgoing[name], AXES, pairs[name]) for name in SENT}
        if step_index == 1:
            arrived["corner"] = kept(live(2), arrived["corner"])
        partial = source_term(second_edges if step_index == 1 else later_sources[step_index, 0, 0])
        for name in ("east", "corner"):
            partial = partial + times(operator[:, rows[name]], arrived[name])
        if step_index == tick_total - 1:
            total = times(operator[:, rows["north"]], arrived["north"]) + partial
            return kept(live(step_index), total)[None, None]
        outgoing, previous = {}, arrived["north"]
        for name in SENT:
            product = times(operator[rows[name], rows["north"]], previous) + partial[rows[name]]
            sent = has_target[name] & live(step_index) if name == "corner" else has_target[name]
            outgoing[name] = kept(sent, product).astype(jnp.bfloat16)
            previous = after(arrived["north"], outgoing[name])


def solution(mesh):
    pairs = {
        "east": shift_pairs(mesh, 1, 0),
        "north": shift_pairs(mesh, 0, 1),
        "corner": diagonal_pairs(mesh),
    }
    in_specs = (
        P("gx", "gy", None, None),
        P(None, "gx", "gy", None, None),
        P("gx", "gy", None, None),
        P(),
    )

    def body(*shards):
        return local(pairs, *shards)

    return jax.shard_map(body, mesh=mesh, in_specs=in_specs, out_specs=P("gx", "gy", None, None), check_vma=False)
```

```python
import random

import jax
import jax.numpy as jnp
from jax import lax
from jax.experimental import pallas as pl
from jax.experimental.pallas import tpu as pltpu
from jax.sharding import PartitionSpec as P


AXES = ("gx", "gy")
SENT = ("north", "east", "corner")


def distance(mesh, a, b):
    devices = mesh.devices.flat
    place = []
    for k in (a, b):
        coords = getattr(devices[k], "coords", None)
        place.append(divmod(k, mesh.shape["gy"]) if coords is None else tuple(coords))
    return sum(abs(p - q) for p, q in zip(*place))


def shift_pairs(mesh, dx, dy):
    nx, ny = mesh.shape["gx"], mesh.shape["gy"]
    return [(i * ny + j, (i + dx) % nx * ny + (j + dy) % ny) for i in range(nx) for j in range(ny)]


def diagonal_pairs(mesh):
    nx, ny = mesh.shape["gx"], mesh.shape["gy"]
    inner = [(i * ny + j, (i + 1) * ny + j + 1) for i in range(nx - 1) for j in range(ny - 1)]
    onward = dict(inner)
    arrived = set(onward.values())
    starts = [k for k in range(nx * ny) if k not in arrived]
    ends = []
    for k in starts:
        while k in onward:
            k = onward[k]
        ends.append(k)
    total = len(starts)
    gap = [[distance(mesh, e, s) for s in starts] for e in ends]

    def cost(order):
        hops = [gap[order[k - 1]][order[k]] for k in range(total)]
        return max(hops), sum(h * h for h in hops)

    draw = random.Random(1)
    best = None
    for _ in range(max(1, 6000 // total**2)):
        order = list(range(total))
        draw.shuffle(order)
        current = cost(order)
        moved = True
        while moved:
            moved = False
            for a in range(total):
                for b in range(a + 1, total):
                    swapped = order[:]
                    swapped[a], swapped[b] = swapped[b], swapped[a]
                    slid = order[:a] + order[a + 1 : b + 1] + [order[a]] + order[b + 1 :]
                    for trial in (swapped, slid):
                        value = cost(trial)
                        if value < current:
                            order, current, moved = trial, value, True
        if best is None or current < best[0]:
            best = current, order
    order = best[1]
    return inner + [(ends[order[k - 1]], starts[order[k]]) for k in range(total)]


def after(value, *others):
    return lax.optimization_barrier((value, *others))[0]


def trace_slices(order, edge_rows):
    trace_rows = edge_rows // 2
    return {
        "east": slice(0, trace_rows),
        "north": slice(trace_rows, edge_rows),
        "corner": slice(edge_rows, order),
    }


def targets():
    east = lax.axis_index("gx") < lax.axis_size("gx") - 1
    north = lax.axis_index("gy") < lax.axis_size("gy") - 1
    return {"east": east, "north": north, "corner": east & north}


def first_tick(green, sources, entering):
    order, width = entering.shape[2:]
    edge_rows = sources.shape[3]
    rows = trace_slices(order, edge_rows)

    def kernel(green_hbm, sources_hbm, entering_hbm, north, east, corner, operator, later, edges, wide, narrow, sems):
        outgoing = {"corner": corner, "east": east, "north": north}
        has_target = targets()

        def fetch(source, target, k):
            copy = pltpu.make_async_copy(source, target, sems.at[k])
            copy.start()
            return copy

        entering_copy = fetch(entering_hbm.at[0, 0], wide, 0)
        operator_copies = {}
        for k, name in enumerate(SENT):
            part = pl.ds(rows[name].start, rows[name].stop - rows[name].start)
            operator_copies[name] = fetch(green_hbm.at[0, 0, part], operator.at[part], 1 + k)
            if k == 0:
                edges_copy = fetch(sources_hbm.at[0, 0, 0], edges, 1 + len(SENT))
        later_copy = fetch(sources_hbm.at[1, 0, 0], later, 2 + len(SENT))
        entering_copy.wait()
        narrow[...] = wide[...].astype(jnp.bfloat16)
        for k, name in enumerate(SENT):
            operator_copies[name].wait()
            product = jnp.dot(operator[rows[name]], narrow[...], preferred_element_type=jnp.float32)
            if k == 0:
                edges_copy.wait()
            if name != "corner":
                product = product + edges[rows[name]].astype(jnp.float32)
            outgoing[name][...] = jnp.where(has_target[name], product, 0.0).astype(jnp.bfloat16)
        later_copy.wait()

    count = {name: rows[name].stop - rows[name].start for name in SENT}
    results = [jax.ShapeDtypeStruct((count[name], width), jnp.bfloat16) for name in SENT]
    results += [jax.ShapeDtypeStruct((order, order), jnp.bfloat16), jax.ShapeDtypeStruct((edge_rows, width), jnp.bfloat16)]
    call = pl.pallas_call(
        kernel,
        out_shape=results,
        in_specs=[pl.BlockSpec(memory_space=pltpu.HBM)] * 3,
        out_specs=[pl.BlockSpec(memory_space=pltpu.VMEM)] * len(results),
        scratch_shapes=[
            pltpu.VMEM((edge_rows, width), jnp.bfloat16),
            pltpu.VMEM((order, width), jnp.float32),
            pltpu.VMEM((order, width), jnp.bfloat16),
            pltpu.SemaphoreType.DMA((3 + len(SENT),)),
        ],
        compiler_params=pltpu.CompilerParams(vmem_limit_bytes=46_000_000),
        cost_estimate=pl.CostEstimate(
            flops=2 * order * order * width,
            bytes_accessed=2 * order * order + 4 * order * width + 4 * edge_rows * width,
            transcendentals=0,
        ),
        name="first_tick",
    )
    in_hbm = [pltpu.with_memory_space_constraint(value, pltpu.HBM) for value in (green, sources, entering)]
    *outgoing, operator, later = call(*in_hbm)
    return dict(zip(SENT, outgoing)), operator, later


def local(pairs, green, sources, entering, start_front):
    tick_total = sources.shape[0]
    order, width = entering.shape[2:]
    edge_rows = sources.shape[3]
    rows = trace_slices(order, edge_rows)
    front_index = lax.axis_index("gx") + lax.axis_index("gy")
    has_target = targets()

    def times(matrix, vectors):
        return jnp.dot(matrix, vectors, preferred_element_type=jnp.float32)

    def source_term(edges):
        return jnp.concatenate(
            [edges.astype(jnp.float32), jnp.zeros((order - edge_rows, width), jnp.float32)], axis=0
        )

    def kept(condition, value):
        return jnp.where(condition, value, jnp.zeros_like(value))

    outgoing, operator, second_edges = first_tick(green, sources, entering)

    span = max(tick_total, 3)
    age = front_index - after(start_front, outgoing["north"])
    live_bits = lax.reduce(
        jnp.where((age >= 0) & (age < span), lax.shift_left(jnp.int32(1), jnp.clip(age, 0, span - 1)), 0),
        jnp.int32(0),
        lax.bitwise_or,
        (0,),
    )
    live_bits = live_bits | (front_index << span)
    later_sources = after(sources, outgoing["north"])

    def live(step_index):
        return (lax.shift_right_logical(live_bits, jnp.int32(step_index)) & 1) == 1

    for step_index in range(1, tick_total):
        arrived = {}
        for name in SENT:
            arrived[name] = lax.ppermute(outgoing[name], AXES, pairs[name])
        if step_index == 1:
            arrived["corner"] = kept(live(2), arrived["corner"])
        partial = source_term(second_edges if step_index == 1 else later_sources[step_index, 0, 0])
        for name in SENT[-2::-1]:
            partial = partial + times(operator[:, rows[name]], arrived[name])
        total = times(operator[:, rows[SENT[-1]]], arrived[SENT[-1]]) + partial
        if step_index == tick_total - 1:
            return kept(live(step_index), total)[None, None]
        for name in SENT:
            sent = has_target[name] & live(step_index) if name == "corner" else has_target[name]
            outgoing[name] = kept(sent, total[rows[name]]).astype(jnp.bfloat16)


def solution(mesh):
    pairs = {
        "east": shift_pairs(mesh, 1, 0),
        "north": shift_pairs(mesh, 0, 1),
        "corner": diagonal_pairs(mesh),
    }
    in_specs = (
        P("gx", "gy", None, None),
        P(None, "gx", "gy", None, None),
        P("gx", "gy", None, None),
        P(),
    )

    def body(*shards):
        return local(pairs, *shards)

    return jax.shard_map(body, mesh=mesh, in_specs=in_specs, out_specs=P("gx", "gy", None, None), check_vma=False)
```
